32 devices in a mesh: slab: 2 (over x), row: 16 (over z, y, core).
Axes of the slice: x: 2, y: 2, z: 4, core: 2. Of those that a mesh axis runs over, the one named last changes fastest.
Arguments:
- raw_echo: float32 [2, 1024, 16384], P(None, 'slab', 'row'), parts along dimension 1, may hold values from -6 to 6
- centroid: int32 [8], P('slab'), parts along dimension 0, may hold values from 0 to 16383
- shifts: int32 [8], P('slab'), parts along dimension 0, may hold values from 0 to 12, as said below
- chirp_rate: float32 [1024], P(('slab', 'row')), parts along dimension 0, may hold values from 50 to 400
Outputs:
- focused_image: float32 [2, 1024, 16384], P(None, ('slab', 'row')), parts along dimension 1
The draws below stay inside these ranges and needn't reach their ends.
There are 2 independent parts, one for each index of `slab`. The reference program is written for one: setup_inputs(seed, part) draws one part's arguments, and reference() takes and returns one part's arrays. A program takes and returns all parts, laid end to end along the dimension named above; each array names one. Nothing has to cross between parts.
Inputs may be any that keep to these rules, and one draw needn't show every extreme that they name: `shifts`: range migration of each block in range bins; some block reaches 12 in every draw.
All inputs are finite; a program needn't handle non-finite values.
Results may differ from the reference program's by a relative error of at most 0.0003.
Values sent between devices are 32-bit elements; how exact they have to be, the bound alone decides.
A program may use at most 128 MiB of HBM per device.

```python
import math
import jax
import jax.numpy as jnp
from jax import lax

PULSES = 16384
RANGE = 512
BLOCK = 128
MAXSHIFT = 12
TAPS = 4


def slab_plan(key):
    block_count = RANGE // BLOCK
    block_ids = jnp.arange(block_count, dtype=jnp.int32)
    chosen = jax.random.randint(jax.random.fold_in(key, 23), (), 0, block_count, dtype=jnp.int32)
    shift_draw = jax.random.randint(jax.random.fold_in(key, 11), (block_count,), 0, MAXSHIFT + 1, dtype=jnp.int32)
    shift_values = jnp.where(block_ids == chosen, MAXSHIFT, shift_draw)
    center_draw = jax.random.randint(jax.random.fold_in(key, 37), (block_count,), 0, PULSES, dtype=jnp.int32)
    edge_center = 8 * jax.random.randint(jax.random.fold_in(key, 41), (), 0, PULSES // 8, dtype=jnp.int32) + 4
    centers = jnp.where(block_ids == chosen, edge_center, center_draw)
    return (centers, shift_values, chosen, edge_center)


def draw_centroid(key, part):
    return slab_plan(key)[0]


def draw_shifts(key, part):
    return slab_plan(key)[1]


def draw_raw_echo(key, part):
    centers, shift_values, chosen, edge_center = slab_plan(key)
    noise_key = jax.random.fold_in(key, 53)
    noise = jax.random.truncated_normal(noise_key, -6.0, 6.0, (2, RANGE, PULSES), jnp.float32)
    quarter = BLOCK // 4
    pulse_index = jnp.arange(PULSES, dtype=jnp.int32)
    edge_bin = (edge_center + PULSES // 2) % PULSES
    first_offset = PULSES // 16 + jax.random.randint(jax.random.fold_in(key, 61), (), 0, PULSES // 32 + 1, dtype=jnp.int32)
    candidates = first_offset + jnp.arange(PULSES // 16, dtype=jnp.int32)
    ratio = candidates.astype(jnp.float32) / PULSES
    scaled = 32.0 * MAXSHIFT * 4.0 * ratio * ratio
    offset_score = jnp.abs(scaled - jnp.floor(scaled) - 0.5)
    distance = candidates[jnp.argmin(offset_score)]
    sign_draw = jnp.where(jax.random.bernoulli(jax.random.fold_in(key, 67)), 1, -1).astype(jnp.int32)
    table_bin = (edge_center + sign_draw * distance) % PULSES
    row_local = jnp.arange(2 * quarter, dtype=jnp.int32)
    bins = jnp.where(row_local < quarter, edge_bin, table_bin)
    edge_phases = jax.random.uniform(jax.random.fold_in(key, 71), (2 * quarter,), jnp.float32, 0.0, 2.0 * math.pi)
    table_phase = jax.random.uniform(jax.random.fold_in(key, 79), (), jnp.float32, 0.0, 2.0 * math.pi)
    alternating = math.pi * (row_local % 2).astype(jnp.float32)
    row_phase = jnp.where(row_local < quarter, edge_phases, table_phase + alternating)
    cycles = (bins[:, None] * pulse_index[None, :] % PULSES).astype(jnp.float32)
    angles = 2.0 * math.pi / PULSES * cycles + row_phase[:, None]
    small_noise = jnp.clip(0.3 * jax.random.normal(jax.random.fold_in(key, 83), (2, 2 * quarter, PULSES), jnp.float32), -1.0, 1.0)
    tones = 5.0 * jnp.stack([jnp.cos(angles), jnp.sin(angles)]) + small_noise
    anchor = jnp.zeros((), jnp.int32)
    start_row = (chosen * BLOCK).astype(jnp.int32)
    return lax.dynamic_update_slice(noise, tones.astype(jnp.float32), (anchor, start_row, anchor))


def block_levels(own_key, dims, pieces, smallest, high):
    factor_of = 1.0
    for dim, blocks in pieces:
        steps = jax.random.uniform(jax.random.fold_in(jax.random.fold_in(own_key, 6), dim), (blocks,), jnp.float32, smallest / len(pieces), high / len(pieces))
        factor_of = factor_of * jnp.repeat(jnp.exp(steps), dims[dim] // blocks).reshape((-1,) + (1,) * (len(dims) - 1 - dim))
    return factor_of


def setup_inputs(seed: int = 0, part: int = 0) -> dict:
    key_of = jax.random.split(jax.random.key(seed), 5)
    part_splits = jax.random.split(jax.random.fold_in(key_of[4], part), 5)
    raw_echo = draw_raw_echo(jax.random.fold_in(jax.random.fold_in(key_of[4], part), 71), part)
    centroid = draw_centroid(jax.random.fold_in(jax.random.fold_in(key_of[4], part), 71), part)
    shifts = draw_shifts(jax.random.fold_in(jax.random.fold_in(key_of[4], part), 71), part)
    chirp_rate = jnp.clip(jnp.exp(math.log(400.0) - 2.0794415 * jax.random.uniform(part_splits[3], (RANGE,), jnp.float32) ** block_levels(part_splits[3], (RANGE,), ((0, 16),), -0.2, 0.2)), 50.0, 400.0)
    return {"raw_echo": raw_echo, "centroid": centroid, "shifts": shifts, "chirp_rate": chirp_rate}


def relative_doppler(center_bin):
    doppler_bins = jnp.arange(PULSES, dtype=jnp.int32)
    wrapped = (doppler_bins - center_bin + PULSES // 2) % PULSES - PULSES // 2
    return wrapped.astype(jnp.float32) / PULSES


def kernel(offsets):
    inside = jnp.abs(offsets) < TAPS
    tapering = jnp.cos(math.pi * offsets / (2.0 * TAPS))
    return jnp.where(inside, jnp.sinc(offsets) * tapering * tapering, 0.0)


def reference(raw_echo, centroid, shifts, chirp_rate):
    lower_rim = TAPS - 1
    upper_rim = MAXSHIFT + TAPS - 1
    padded = jnp.pad(raw_echo, ((0, 0), (lower_rim, upper_rim), (0, 0)))
    extent = BLOCK + lower_rim + upper_rim

    def one_block(block_index):
        first_row = (block_index * BLOCK).astype(jnp.int32)
        anchor = jnp.zeros((), jnp.int32)
        window_rows = lax.dynamic_slice(padded, (anchor, first_row, anchor), (2, extent, PULSES))
        spectrum = jnp.fft.fft(window_rows[0] + 1j * window_rows[1], axis=-1)
        relative = relative_doppler(centroid[block_index])
        migration = shifts[block_index].astype(jnp.float32) * 4.0 * relative * relative
        migrated = kernel(-lower_rim - migration)[None, :] * spectrum[0:BLOCK]
        for offset in range(1 - lower_rim, upper_rim + 1):
            weight = kernel(offset - migration)
            start_row = offset + lower_rim
            migrated = migrated + weight[None, :] * spectrum[start_row:start_row + BLOCK]
        block_rates = lax.dynamic_slice(chirp_rate, (first_row,), (BLOCK,))
        window = 0.54 + 0.46 * jnp.cos(2.0 * math.pi * relative)
        phase_angle = math.pi * block_rates[:, None] * (relative * relative)[None, :]
        focused = migrated * window[None, :] * (jnp.cos(phase_angle) - 1j * jnp.sin(phase_angle))
        picture = jnp.fft.ifft(focused, axis=-1)
        return jnp.stack([jnp.real(picture), jnp.imag(picture)]).astype(jnp.float32)

    blocks = lax.map(one_block, jnp.arange(RANGE // BLOCK, dtype=jnp.int32))
    return jnp.transpose(blocks, (1, 0, 2, 3)).reshape(2, RANGE, PULSES)
```

```python
import functools
import math

import jax
import jax.numpy as jnp
import numpy as np
from jax import lax
from jax.experimental import pallas as pl
from jax.experimental.pallas import tpu as pltpu
from jax.sharding import PartitionSpec as P

FACTOR = 128
PULSES = FACTOR * FACTOR
BLOCK = 128
MAXSHIFT = 12
TAPS = 4
LOWER = TAPS - 1
UPPER = MAXSHIFT + TAPS - 1
GROUP = 8
SUB = 8


def split(value):
    high = value.astype(jnp.bfloat16)
    low = (value - high.astype(jnp.float32)).astype(jnp.bfloat16)
    return high, low


def tables(inverse):
    grid = np.outer(np.arange(FACTOR), np.arange(FACTOR)).astype(np.float64)
    angle = 2.0 * math.pi * (grid % FACTOR) / FACTOR
    scale = 1.0 / FACTOR if inverse else 1.0
    cosine = np.cos(angle) * scale
    sine = np.sin(angle) * scale * (-1.0 if inverse else 1.0)
    left = np.block([[cosine, sine], [-sine, cosine]]).astype(np.float32)
    right = np.block([[cosine, -sine], [sine, cosine]]).astype(np.float32)
    turn = 2.0 * math.pi * grid / PULSES
    twist = np.stack([np.cos(turn), np.sin(turn) * (1.0 if inverse else -1.0)]).astype(np.float32)

    def pieces(table):
        high = table.astype(jnp.bfloat16)
        low = (table - high.astype(np.float32)).astype(jnp.bfloat16)
        return high, low

    left_high, left_low = pieces(left)
    right_high, right_low = pieces(right)
    left_all = np.concatenate([left_high, left_high, left_low], axis=1)
    right_all = np.concatenate([right_high, right_high, right_low], axis=0)
    return jnp.asarray(left_all), jnp.asarray(right_all), jnp.asarray(twist)


def left_product(left_ref, first, second):
    operand = jnp.concatenate(
        [jnp.concatenate([first[0], second[0]], axis=1), jnp.concatenate([first[1], second[1]], axis=1)],
        axis=0,
    )
    high, low = split(operand)
    stacked = jnp.concatenate([high, low, high], axis=0)
    return jnp.dot(left_ref[...], stacked, preferred_element_type=jnp.float32)


def right_product(right_ref, operand):
    high, low = split(operand)
    stacked = jnp.concatenate([high, low, high], axis=1)
    return jnp.dot(stacked, right_ref[...], preferred_element_type=jnp.float32)


def turned(real, imag, twist_ref):
    return real * twist_ref[0] - imag * twist_ref[1], real * twist_ref[1] + imag * twist_ref[0]


def forward_pair(rows, left_ref, right_ref, twist_ref):
    product = left_product(left_ref, rows[0], rows[1])
    parts = []
    for k in range(2):
        lanes = slice(k * FACTOR, (k + 1) * FACTOR)
        real, imag = turned(product[:FACTOR, lanes], product[FACTOR:, lanes], twist_ref)
        parts.append(jnp.concatenate([real, imag], axis=1))
    return right_product(right_ref, jnp.concatenate(parts, axis=0))


def forward_kernel(x_ref, left_ref, right_ref, twist_ref, out_ref, slow):
    sources = x_ref.shape[1]
    pieces = x_ref.shape[3] // FACTOR
    for c in range(2):
        for d in range(sources):
            for j in range(pieces):
                start = (d * pieces + j) * GROUP
                slow[c, start : start + GROUP, :] = x_ref[c, d, :, j * FACTOR : (j + 1) * FACTOR]
    for r in range(0, GROUP, 2):
        rows = [
            [slow[c, pl.ds(r + k, FACTOR, stride=GROUP), :] for c in range(2)] for k in range(2)
        ]
        result = forward_pair(rows, left_ref, right_ref, twist_ref)
        for k in range(2):
            part = result[k * FACTOR : (k + 1) * FACTOR]
            out_ref[0, r + k] = part[:, :FACTOR]
            out_ref[1, r + k] = part[:, FACTOR:]


def half_turns(t):
    n = jnp.round(t)
    w = (t - n) * math.pi
    odd = n - 2.0 * jnp.floor(n * 0.5)
    sign = 1.0 - 2.0 * odd
    w2 = w * w
    sine = w * (1.0 + w2 * (-1 / 6 + w2 * (1 / 120 + w2 * (-1 / 5040 + w2 * (1 / 362880 - w2 * (1 / 39916800))))))
    cosine = 1.0 + w2 * (-0.5 + w2 * (1 / 24 + w2 * (-1 / 720 + w2 * (1 / 40320 - w2 * (1 / 3628800)))))
    return sign, sine, cosine


def relative_of(start, center):
    slow = lax.broadcasted_iota(jnp.int32, (SUB, FACTOR), 0) + start
    fast = lax.broadcasted_iota(jnp.int32, (SUB, FACTOR), 1)
    bins = fast * FACTOR + slow
    wrapped = ((bins - center + PULSES // 2) & (PULSES - 1)) - PULSES // 2
    return wrapped.astype(jnp.float32) * (1.0 / PULSES)


def fill_weights(center, shift, weights, window):
    @pl.loop(0, FACTOR // SUB)
    def _(q):
        start = pl.multiple_of(q * SUB, SUB)
        relative = relative_of(start, center)
        squared = relative * relative
        migration = shift.astype(jnp.float32) * 4.0 * squared
        sign, sine, _c = half_turns(migration)
        sine = sign * sine
        sign4, sine4, cosine4 = half_turns(migration * 0.25)
        sine4 = sign4 * sine4
        cosine4 = sign4 * cosine4
        for s in range(-LOWER, UPPER + 1):
            x = s - migration
            zero = x == 0.0
            numerator = sine * ((1.0 if s % 2 else -1.0) / math.pi)
            sinc = jnp.where(zero, 1.0, numerator / jnp.where(zero, 1.0, x))
            taper = 0.5 + (0.5 * math.cos(math.pi * s / 4)) * cosine4 + (0.5 * math.sin(math.pi * s / 4)) * sine4
            value = jnp.where(jnp.abs(x) < TAPS, sinc * taper, 0.0)
            weights[s + LOWER, pl.ds(start, SUB), :] = value
        wsign, _s, wcos = half_turns(2.0 * relative)
        window[0, pl.ds(start, SUB), :] = 0.54 + 0.46 * (wsign * wcos)
        window[1, pl.ds(start, SUB), :] = squared


def migrate_rows(base, extended, rates_ref, rate_base, weights, window, focus):
    @pl.loop(0, FACTOR // SUB)
    def _(q):
        here = pl.ds(pl.multiple_of(q * SUB, SUB), SUB)
        sums = []
        for c in range(2):
            for r in range(GROUP):
                total = weights[0, here, :] * extended[c, base + r, here, :]
                for s in range(1, LOWER + UPPER + 1):
                    total = total + weights[s, here, :] * extended[c, base + r + s, here, :]
                sums.append(total)
        shape = window[0, here, :]
        squared = window[1, here, :]
        for r in range(GROUP):
            sign, sine, cosine = half_turns(rates_ref[rate_base + r] * squared)
            gain = sign * shape
            real, imag = sums[r] * gain, sums[GROUP + r] * gain
            focus[r, here, :FACTOR] = real * cosine + imag * sine
            focus[r, here, FACTOR:] = imag * cosine - real * sine


def inverse_group(focus, left_ref, right_ref, twist_ref, slow, out_ref):
    for r in range(0, GROUP, 2):
        operand = jnp.concatenate([focus[r], focus[r + 1]], axis=0)
        product = right_product(right_ref, operand)
        rows = []
        for k in range(2):
            part = product[k * FACTOR : (k + 1) * FACTOR]
            rows.append(turned(part[:, :FACTOR], part[:, FACTOR:], twist_ref))
        result = left_product(left_ref, rows[0], rows[1])
        for k in range(2):
            lanes = slice(k * FACTOR, (k + 1) * FACTOR)
            for c in range(2):
                slow[c, pl.ds(r + k, FACTOR, stride=GROUP), :] = result[c * FACTOR : (c + 1) * FACTOR, lanes]
    for c in range(2):
        for n in range(FACTOR):
            out_ref[c, :, n * FACTOR : (n + 1) * FACTOR] = slow[c, n * GROUP : (n + 1) * GROUP, :]


def backward_kernel(
    place_ref, rates_ref, own_ref, above_ref, below_ref, left_ref, right_ref, twist_ref,
    out_ref, extended, weights, window, focus, slow, sems,
):
    step = pl.program_id(0)
    own_rows = own_ref.shape[1]

    @pl.when(step == 0)
    def _():
        copies = [
            pltpu.make_async_copy(below_ref, extended.at[:, 0:LOWER], sems.at[0]),
            pltpu.make_async_copy(own_ref, extended.at[:, LOWER : LOWER + own_rows], sems.at[1]),
            pltpu.make_async_copy(above_ref, extended.at[:, LOWER + own_rows : LOWER + own_rows + UPPER], sems.at[2]),
        ]
        for copy in copies:
            copy.start()
        fill_weights(place_ref[0], place_ref[1], weights, window)
        for copy in copies:
            copy.wait()

    base = step * GROUP
    migrate_rows(base, extended, rates_ref, base, weights, window, focus)
    inverse_group(focus, left_ref, right_ref, twist_ref, slow, out_ref)


def backward(place, rates, own, above, below):
    own_rows = own.shape[1]
    left, right, twist = tables(True)
    vmem = pl.BlockSpec(memory_space=pltpu.VMEM)
    smem = pl.BlockSpec(memory_space=pltpu.SMEM)
    hbm = pl.BlockSpec(memory_space=pl.ANY)
    return pl.pallas_call(
        backward_kernel,
        grid=(own_rows // GROUP,),
        in_specs=[smem, smem, hbm, hbm, hbm, vmem, vmem, vmem],
        out_specs=pl.BlockSpec((2, GROUP, PULSES), lambda g: (0, g, 0)),
        out_shape=jax.ShapeDtypeStruct((2, own_rows, PULSES), jnp.float32),
        scratch_shapes=[
            pltpu.VMEM((2, own_rows + LOWER + UPPER, FACTOR, FACTOR), jnp.float32),
            pltpu.VMEM((LOWER + UPPER + 1, FACTOR, FACTOR), jnp.float32),
            pltpu.VMEM((2, FACTOR, FACTOR), jnp.float32),
            pltpu.VMEM((GROUP, FACTOR, 2 * FACTOR), jnp.float32),
            pltpu.VMEM((2, FACTOR * GROUP, FACTOR), jnp.float32),
            pltpu.SemaphoreType.DMA((3,)),
        ],
        compiler_params=pltpu.CompilerParams(vmem_limit_bytes=40 * 2**20),
    )(place, rates, own, above, below, left, right, twist)


def forward(x):
    devices, own_rows, share = x.shape[1:]
    left, right, twist = tables(False)
    vmem = pl.BlockSpec(memory_space=pltpu.VMEM)
    return pl.pallas_call(
        forward_kernel,
        grid=(own_rows // GROUP,),
        in_specs=[pl.BlockSpec((2, devices, GROUP, share), lambda g: (0, 0, g, 0)), vmem, vmem, vmem],
        out_specs=pl.BlockSpec((2, GROUP, FACTOR, FACTOR), lambda g: (0, g, 0, 0)),
        out_shape=jax.ShapeDtypeStruct((2, own_rows, FACTOR, FACTOR), jnp.float32),
        scratch_shapes=[pltpu.VMEM((2, FACTOR * GROUP, FACTOR), jnp.float32)],
        compiler_params=pltpu.CompilerParams(vmem_limit_bytes=40 * 2**20),
    )(x, left, right, twist)


def from_behind(shard, axis, by):
    devices = lax.axis_size(axis)
    pairs = [(i, i + by) for i in range(devices) if 0 <= i + by < devices]
    return lax.ppermute(shard, axis, pairs)


def place_of(centroid, shifts, own_rows):
    block = lax.axis_index("row") * own_rows // BLOCK
    chosen = block == jnp.arange(centroid.shape[0], dtype=jnp.int32)
    return jnp.stack([jnp.sum(jnp.where(chosen, centroid, 0)), jnp.sum(jnp.where(chosen, shifts, 0))])


def per_device(raw_echo, centroid, shifts, chirp_rate):
    devices = lax.axis_size("row")
    own_rows = raw_echo.shape[1] // devices
    share = raw_echo.shape[2]
    assert BLOCK % own_rows == 0 and own_rows % GROUP == 0 and own_rows >= UPPER
    place = place_of(centroid, shifts, own_rows)
    blocks = raw_echo.reshape(2, devices, own_rows, share)
    gathered = lax.all_to_all(blocks, "row", split_axis=1, concat_axis=1, tiled=True)
    spectrum = forward(gathered)
    above = from_behind(spectrum[:, :UPPER], "row", -1)
    below = from_behind(spectrum[:, own_rows - LOWER :], "row", 1)
    return backward(place, chirp_rate, spectrum, above, below)


def solution(mesh):
    return jax.shard_map(
        per_device,
        mesh=mesh,
        in_specs=(P(None, "slab", "row"), P("slab"), P("slab"), P(("slab", "row"))),
        out_specs=P(None, ("slab", "row"), None),
        check_vma=False,
    )
```

```python
import functools
import math

import jax
import jax.numpy as jnp
import numpy as np
from jax import lax
from jax.experimental import pallas as pl
from jax.experimental.pallas import tpu as pltpu
from jax.sharding import PartitionSpec as P

FACTOR = 128
PULSES = FACTOR * FACTOR
BLOCK = 128
MAXSHIFT = 12
TAPS = 4
LOWER = TAPS - 1
UPPER = MAXSHIFT + TAPS - 1
GROUP = 8
SUB = 8


def split(value):
    high = value.astype(jnp.bfloat16)
    low = (value - high.astype(jnp.float32)).astype(jnp.bfloat16)
    return high, low


def tables(inverse):
    grid = np.outer(np.arange(FACTOR), np.arange(FACTOR)).astype(np.float64)
    angle = 2.0 * math.pi * (grid % FACTOR) / FACTOR
    scale = 1.0 / FACTOR if inverse else 1.0
    cosine = np.cos(angle) * scale
    sine = np.sin(angle) * scale * (-1.0 if inverse else 1.0)
    left = np.block([[cosine, sine], [-sine, cosine]]).astype(np.float32)
    right = np.block([[cosine, -sine], [sine, cosine]]).astype(np.float32)
    turn = 2.0 * math.pi * grid / PULSES
    twist = np.stack([np.cos(turn), np.sin(turn) * (1.0 if inverse else -1.0)]).astype(np.float32)

    def pieces(table):
        high = table.astype(jnp.bfloat16)
        low = (table - high.astype(np.float32)).astype(jnp.bfloat16)
        return high, low

    left_high, left_low = pieces(left)
    right_high, right_low = pieces(right)
    left_all = np.concatenate([left_high, left_high, left_low], axis=1)
    right_all = np.concatenate([right_high, right_high, right_low], axis=0)
    return jnp.asarray(left_all), jnp.asarray(right_all), jnp.asarray(twist)


def left_product(left_ref, first, second):
    operand = jnp.concatenate(
        [jnp.concatenate([first[0], second[0]], axis=1), jnp.concatenate([first[1], second[1]], axis=1)],
        axis=0,
    )
    high, low = split(operand)
    stacked = jnp.concatenate([high, low, high], axis=0)
    return jnp.dot(left_ref[...], stacked, preferred_element_type=jnp.float32)


def right_product(right_ref, operand):
    high, low = split(operand)
    stacked = jnp.concatenate([high, low, high], axis=1)
    return jnp.dot(stacked, right_ref[...], preferred_element_type=jnp.float32)


def turned(real, imag, twist_ref):
    return real * twist_ref[0] - imag * twist_ref[1], real * twist_ref[1] + imag * twist_ref[0]


def forward_pair(rows, left_ref, right_ref, twist_ref):
    product = left_product(left_ref, rows[0], rows[1])
    parts = []
    for k in range(2):
        lanes = slice(k * FACTOR, (k + 1) * FACTOR)
        real, imag = turned(product[:FACTOR, lanes], product[FACTOR:, lanes], twist_ref)
        parts.append(jnp.concatenate([real, imag], axis=1))
    return right_product(right_ref, jnp.concatenate(parts, axis=0))


def half_turns(t):
    n = jnp.round(t)
    w = (t - n) * math.pi
    odd = n - 2.0 * jnp.floor(n * 0.5)
    sign = 1.0 - 2.0 * odd
    w2 = w * w
    sine = w * (1.0 + w2 * (-1 / 6 + w2 * (1 / 120 + w2 * (-1 / 5040 + w2 * (1 / 362880 - w2 * (1 / 39916800))))))
    cosine = 1.0 + w2 * (-0.5 + w2 * (1 / 24 + w2 * (-1 / 720 + w2 * (1 / 40320 - w2 * (1 / 3628800)))))
    return sign, sine, cosine


def relative_of(start, center):
    slow = lax.broadcasted_iota(jnp.int32, (SUB, FACTOR), 0) + start
    fast = lax.broadcasted_iota(jnp.int32, (SUB, FACTOR), 1)
    bins = fast * FACTOR + slow
    wrapped = ((bins - center + PULSES // 2) & (PULSES - 1)) - PULSES // 2
    return wrapped.astype(jnp.float32) * (1.0 / PULSES)


def fill_weights(center, shift, weights, window):
    @pl.loop(0, FACTOR // SUB)
    def _(q):
        start = pl.multiple_of(q * SUB, SUB)
        relative = relative_of(start, center)
        squared = relative * relative
        migration = shift.astype(jnp.float32) * 4.0 * squared
        sign, sine, _c = half_turns(migration)
        sine = sign * sine
        sign4, sine4, cosine4 = half_turns(migration * 0.25)
        sine4 = sign4 * sine4
        cosine4 = sign4 * cosine4
        for s in range(-LOWER, UPPER + 1):
            x = s - migration
            zero = x == 0.0
            numerator = sine * ((1.0 if s % 2 else -1.0) / math.pi)
            sinc = jnp.where(zero, 1.0, numerator / jnp.where(zero, 1.0, x))
            taper = 0.5 + (0.5 * math.cos(math.pi * s / 4)) * cosine4 + (0.5 * math.sin(math.pi * s / 4)) * sine4
            value = jnp.where(jnp.abs(x) < TAPS, sinc * taper, 0.0)
            weights[s + LOWER, pl.ds(start, SUB), :] = value
        wsign, _s, wcos = half_turns(2.0 * relative)
        window[0, pl.ds(start, SUB), :] = 0.54 + 0.46 * (wsign * wcos)
        window[1, pl.ds(start, SUB), :] = squared


def migrate_rows(base, extended, rates_ref, rate_base, weights, window, focus):
    @pl.loop(0, FACTOR // SUB)
    def _(q):
        here = pl.ds(pl.multiple_of(q * SUB, SUB), SUB)
        sums = []
        for c in range(2):
            for r in range(GROUP):
                total = weights[0, here, :] * extended[c, base + r, here, :]
                for s in range(1, LOWER + UPPER + 1):
                    total = total + weights[s, here, :] * extended[c, base + r + s, here, :]
                sums.append(total)
        shape = window[0, here, :]
        squared = window[1, here, :]
        for r in range(GROUP):
            sign, sine, cosine = half_turns(rates_ref[rate_base + r] * squared)
            gain = sign * shape
            real, imag = sums[r] * gain, sums[GROUP + r] * gain
            focus[r, here, :FACTOR] = real * cosine + imag * sine
            focus[r, here, FACTOR:] = imag * cosine - real * sine


def inverse_group(focus, left_ref, right_ref, twist_ref, slow, out_ref):
    for r in range(0, GROUP, 2):
        operand = jnp.concatenate([focus[r], focus[r + 1]], axis=0)
        product = right_product(right_ref, operand)
        rows = []
        for k in range(2):
            part = product[k * FACTOR : (k + 1) * FACTOR]
            rows.append(turned(part[:, :FACTOR], part[:, FACTOR:], twist_ref))
        result = left_product(left_ref, rows[0], rows[1])
        for k in range(2):
            lanes = slice(k * FACTOR, (k + 1) * FACTOR)
            for c in range(2):
                slow[c, pl.ds(r + k, FACTOR, stride=GROUP), :] = result[c * FACTOR : (c + 1) * FACTOR, lanes]
    for c in range(2):
        for n in range(FACTOR):
            out_ref[c, :, n * FACTOR : (n + 1) * FACTOR] = slow[c, n * GROUP : (n + 1) * GROUP, :]


def backward_kernel(
    place_ref, rates_ref, wide_ref, left_ref, right_ref, twist_ref,
    out_ref, extended, weights, window, focus, slow, sems,
):
    step = pl.program_id(0)
    steps = extended.shape[1] // GROUP - (LOWER + UPPER) // GROUP
    lead = GROUP + LOWER + UPPER

    def piece(g):
        rows = pl.ds(0, lead) if g == 0 else pl.ds(lead + (g - 1) * GROUP, GROUP)
        return pltpu.make_async_copy(wide_ref.at[:, rows], extended.at[:, rows], sems.at[g])

    @pl.when(step == 0)
    def _():
        for g in range(steps):
            piece(g).start()
        fill_weights(place_ref[0], place_ref[1], weights, window)

    for g in range(steps):
        @pl.when(step == g)
        def _():
            piece(g).wait()

    base = step * GROUP
    migrate_rows(base, extended, rates_ref, base, weights, window, focus)
    inverse_group(focus, left_ref, right_ref, twist_ref, slow, out_ref)


def backward(place, rates, wide):
    own_rows = wide.shape[1] - LOWER - UPPER
    left, right, twist = tables(True)
    vmem = pl.BlockSpec(memory_space=pltpu.VMEM)
    smem = pl.BlockSpec(memory_space=pltpu.SMEM)
    hbm = pl.BlockSpec(memory_space=pl.ANY)
    return pl.pallas_call(
        backward_kernel,
        grid=(own_rows // GROUP,),
        in_specs=[smem, smem, hbm, vmem, vmem, vmem],
        out_specs=pl.BlockSpec((2, GROUP, PULSES), lambda g: (0, g, 0)),
        out_shape=jax.ShapeDtypeStruct((2, own_rows, PULSES), jnp.float32),
        scratch_shapes=[
            pltpu.VMEM((2, own_rows + LOWER + UPPER, FACTOR, FACTOR), jnp.float32),
            pltpu.VMEM((LOWER + UPPER + 1, FACTOR, FACTOR), jnp.float32),
            pltpu.VMEM((2, FACTOR, FACTOR), jnp.float32),
            pltpu.VMEM((GROUP, FACTOR, 2 * FACTOR), jnp.float32),
            pltpu.VMEM((2, FACTOR * GROUP, FACTOR), jnp.float32),
            pltpu.SemaphoreType.DMA((own_rows // GROUP,)),
        ],
        compiler_params=pltpu.CompilerParams(vmem_limit_bytes=40 * 2**20),
    )(place, rates, wide, left, right, twist)


def gather_kernel(
    devices, raw_ref, left_ref, right_ref, twist_ref, wide_ref,
    landed, extended, slow, send_sem, recv_sems, self_sem, out_sems, rim_send, rim_recv,
):
    me = lax.axis_index("row")
    own_rows = landed.shape[2]
    groups = own_rows // GROUP
    pieces = landed.shape[3] // FACTOR

    barrier = pltpu.get_barrier_semaphore()

    @pl.loop(1, devices)
    def _(k):
        pl.semaphore_signal(barrier, inc=1, device_id={"row": (me + k) % devices})

    pl.semaphore_wait(barrier, devices - 1)

    own = pltpu.make_async_copy(raw_ref.at[:, pl.ds(me * own_rows, own_rows)], landed.at[:, me], self_sem)
    own.start()
    for g in range(groups):
        @pl.loop(1, devices)
        def _(k):
            peer = (me + k) % devices
            pltpu.make_async_remote_copy(
                src_ref=raw_ref.at[:, pl.ds(peer * own_rows + g * GROUP, GROUP)],
                dst_ref=landed.at[:, me, pl.ds(g * GROUP, GROUP)],
                send_sem=send_sem,
                recv_sem=recv_sems.at[g],
                device_id={"row": peer},
            ).start()

    @pl.when(me == 0)
    def _():
        extended[:, 0:LOWER] = jnp.zeros((2, LOWER, FACTOR, FACTOR), jnp.float32)

    @pl.when(me == devices - 1)
    def _():
        extended[:, LOWER + own_rows :] = jnp.zeros((2, UPPER, FACTOR, FACTOR), jnp.float32)

    own.wait()

    def rim_copy(first, count, target, where, slot):
        return pltpu.make_async_remote_copy(
            src_ref=extended.at[:, LOWER + first : LOWER + first + count],
            dst_ref=extended.at[:, where : where + count],
            send_sem=rim_send.at[slot],
            recv_sem=rim_recv.at[slot],
            device_id={"row": target},
        )

    above = rim_copy(0, UPPER, jnp.maximum(me - 1, 0), LOWER + own_rows, 0)
    below = rim_copy(own_rows - LOWER, LOWER, jnp.minimum(me + 1, devices - 1), 0, 1)

    def written(g):
        rows = pl.ds(LOWER + g * GROUP, GROUP)
        return pltpu.make_async_copy(extended.at[:, rows], wide_ref.at[:, rows], out_sems.at[g])

    def arrive_and_transform(g):
        chunk = landed.at[:, 0 : devices - 1, pl.ds(g * GROUP, GROUP)]
        pltpu.make_async_copy(chunk, chunk, recv_sems.at[g]).wait()
        rows = pl.ds(pl.multiple_of(g * GROUP, GROUP), GROUP)
        for c in range(2):
            for d in range(devices):
                for j in range(pieces):
                    start = (d * pieces + j) * GROUP
                    slow[c, start : start + GROUP, :] = landed[c, d, rows, j * FACTOR : (j + 1) * FACTOR]
        for r in range(0, GROUP, 2):
            pair = [
                [slow[c, pl.ds(r + k, FACTOR, stride=GROUP), :] for c in range(2)] for k in range(2)
            ]
            result = forward_pair(pair, left_ref, right_ref, twist_ref)
            for k in range(2):
                part = result[k * FACTOR : (k + 1) * FACTOR]
                extended[0, LOWER + g * GROUP + r + k] = part[:, :FACTOR]
                extended[1, LOWER + g * GROUP + r + k] = part[:, FACTOR:]
        written(g).start()

    first = -(-UPPER // GROUP)

    @pl.loop(0, first)
    def _(g):
        arrive_and_transform(g)

    @pl.when(me > 0)
    def _():
        above.start()

    @pl.loop(first, groups)
    def _(g):
        arrive_and_transform(g)

    @pl.when(me < devices - 1)
    def _():
        below.start()

    everything = landed.at[:, 0 : devices - 1]
    pltpu.make_async_copy(everything, everything, send_sem).wait()

    @pl.when(me > 0)
    def _():
        above.wait_send()
        below.wait_recv()

    @pl.when(me < devices - 1)
    def _():
        below.wait_send()
        above.wait_recv()

    rims = [
        pltpu.make_async_copy(extended.at[:, 0:LOWER], wide_ref.at[:, 0:LOWER], out_sems.at[groups]),
        pltpu.make_async_copy(
            extended.at[:, LOWER + own_rows :], wide_ref.at[:, LOWER + own_rows :], out_sems.at[groups + 1]
        ),
    ]
    for rim in rims:
        rim.start()
    for g in range(groups):
        written(g).wait()
    for rim in rims:
        rim.wait()


def gather_forward(raw, devices):
    own_rows = raw.shape[1] // devices
    share = raw.shape[2]
    groups = own_rows // GROUP
    wide_shape = (2, own_rows + LOWER + UPPER, FACTOR, FACTOR)
    left, right, twist = tables(False)
    vmem = pl.BlockSpec(memory_space=pltpu.VMEM)
    hbm = pl.BlockSpec(memory_space=pl.ANY)
    return pl.pallas_call(
        functools.partial(gather_kernel, devices),
        in_specs=[hbm, vmem, vmem, vmem],
        out_specs=hbm,
        out_shape=jax.ShapeDtypeStruct(wide_shape, jnp.float32),
        scratch_shapes=[
            pltpu.VMEM((2, devices, own_rows, share), jnp.float32),
            pltpu.VMEM(wide_shape, jnp.float32),
            pltpu.VMEM((2, FACTOR * GROUP, FACTOR), jnp.float32),
            pltpu.SemaphoreType.DMA,
            pltpu.SemaphoreType.DMA((groups,)),
            pltpu.SemaphoreType.DMA,
            pltpu.SemaphoreType.DMA((groups + 2,)),
            pltpu.SemaphoreType.DMA((2,)),
            pltpu.SemaphoreType.DMA((2,)),
        ],
        compiler_params=pltpu.CompilerParams(
            collective_id=0, has_side_effects=True, vmem_limit_bytes=40 * 2**20
        ),
    )(raw, left, right, twist)


def place_of(centroid, shifts, own_rows):
    block = lax.axis_index("row") * own_rows // BLOCK
    chosen = block == jnp.arange(centroid.shape[0], dtype=jnp.int32)
    return jnp.stack([jnp.sum(jnp.where(chosen, centroid, 0)), jnp.sum(jnp.where(chosen, shifts, 0))])


def per_device(raw_echo, centroid, shifts, chirp_rate):
    devices = lax.axis_size("row")
    own_rows = raw_echo.shape[1] // devices
    assert BLOCK % own_rows == 0 and own_rows % GROUP == 0 and own_rows >= UPPER
    place = place_of(centroid, shifts, own_rows)
    wide = gather_forward(raw_echo, devices)
    return backward(place, chirp_rate, wide)


def solution(mesh):
    return jax.shard_map(
        per_device,
        mesh=mesh,
        in_specs=(P(None, "slab", "row"), P("slab"), P("slab"), P(("slab", "row"))),
        out_specs=P(None, ("slab", "row"), None),
        check_vma=False,
    )
```

```python
import functools
import math

import jax
import jax.numpy as jnp
import numpy as np
from jax import lax
from jax.experimental import pallas as pl
from jax.experimental.pallas import tpu as pltpu
from jax.sharding import PartitionSpec as P

FACTOR = 128
PULSES = FACTOR * FACTOR
BLOCK = 128
MAXSHIFT = 12
TAPS = 4
LOWER = TAPS - 1
UPPER = MAXSHIFT + TAPS - 1
GROUP = 8
SUB = 8


def split(value):
    high = value.astype(jnp.bfloat16)
    low = (value - high.astype(jnp.float32)).astype(jnp.bfloat16)
    return high, low


def tables(inverse):
    grid = np.outer(np.arange(FACTOR), np.arange(FACTOR)).astype(np.float64)
    angle = 2.0 * math.pi * (grid % FACTOR) / FACTOR
    scale = 1.0 / FACTOR if inverse else 1.0
    cosine = np.cos(angle) * scale
    sine = np.sin(angle) * scale * (-1.0 if inverse else 1.0)
    left = np.block([[cosine, sine], [-sine, cosine]]).astype(np.float32)
    right = np.block([[cosine, -sine], [sine, cosine]]).astype(np.float32)
    turn = 2.0 * math.pi * grid / PULSES
    twist = np.stack([np.cos(turn), np.sin(turn) * (1.0 if inverse else -1.0)]).astype(np.float32)

    def pieces(table):
        high = table.astype(jnp.bfloat16)
        low = (table - high.astype(np.float32)).astype(jnp.bfloat16)
        return high, low

    left_high, left_low = pieces(left)
    right_high, right_low = pieces(right)
    left_all = np.concatenate([left_high, left_high, left_low], axis=1)
    right_all = np.concatenate([right_high, right_high, right_low], axis=0)
    return jnp.asarray(left_all), jnp.asarray(right_all), jnp.asarray(twist)


def left_product(left_ref, first, second):
    operand = jnp.concatenate(
        [jnp.concatenate([first[0], second[0]], axis=1), jnp.concatenate([first[1], second[1]], axis=1)],
        axis=0,
    )
    high, low = split(operand)
    stacked = jnp.concatenate([high, low, high], axis=0)
    return jnp.dot(left_ref[...], stacked, preferred_element_type=jnp.float32)


def right_product(right_ref, operand):
    high, low = split(operand)
    stacked = jnp.concatenate([high, low, high], axis=1)
    return jnp.dot(stacked, right_ref[...], preferred_element_type=jnp.float32)


def turned(real, imag, twist_ref):
    return real * twist_ref[0] - imag * twist_ref[1], real * twist_ref[1] + imag * twist_ref[0]


def forward_pair(rows, left_ref, right_ref, twist_ref):
    product = left_product(left_ref, rows[0], rows[1])
    parts = []
    for k in range(2):
        lanes = slice(k * FACTOR, (k + 1) * FACTOR)
        real, imag = turned(product[:FACTOR, lanes], product[FACTOR:, lanes], twist_ref)
        parts.append(jnp.concatenate([real, imag], axis=1))
    return right_product(right_ref, jnp.concatenate(parts, axis=0))


def half_turns(t):
    n = jnp.round(t)
    w = (t - n) * math.pi
    odd = n - 2.0 * jnp.floor(n * 0.5)
    sign = 1.0 - 2.0 * odd
    w2 = w * w
    sine = w * (1.0 + w2 * (-1 / 6 + w2 * (1 / 120 + w2 * (-1 / 5040 + w2 * (1 / 362880 - w2 * (1 / 39916800))))))
    cosine = 1.0 + w2 * (-0.5 + w2 * (1 / 24 + w2 * (-1 / 720 + w2 * (1 / 40320 - w2 * (1 / 3628800)))))
    return sign, sine, cosine


def relative_of(start, center):
    slow = lax.broadcasted_iota(jnp.int32, (SUB, FACTOR), 0) + start
    fast = lax.broadcasted_iota(jnp.int32, (SUB, FACTOR), 1)
    bins = fast * FACTOR + slow
    wrapped = ((bins - center + PULSES // 2) & (PULSES - 1)) - PULSES // 2
    return wrapped.astype(jnp.float32) * (1.0 / PULSES)


def fill_weights(center, shift, weights, window):
    @pl.loop(0, FACTOR // SUB)
    def _(q):
        start = pl.multiple_of(q * SUB, SUB)
        relative = relative_of(start, center)
        squared = relative * relative
        migration = shift.astype(jnp.float32) * 4.0 * squared
        sign, sine, _c = half_turns(migration)
        sine = sign * sine
        sign4, sine4, cosine4 = half_turns(migration * 0.25)
        sine4 = sign4 * sine4
        cosine4 = sign4 * cosine4
        for s in range(-LOWER, UPPER + 1):
            x = s - migration
            zero = x == 0.0
            numerator = sine * ((1.0 if s % 2 else -1.0) / math.pi)
            sinc = jnp.where(zero, 1.0, numerator / jnp.where(zero, 1.0, x))
            taper = 0.5 + (0.5 * math.cos(math.pi * s / 4)) * cosine4 + (0.5 * math.sin(math.pi * s / 4)) * sine4
            value = jnp.where(jnp.abs(x) < TAPS, sinc * taper, 0.0)
            weights[s + LOWER, pl.ds(start, SUB), :] = value
        wsign, _s, wcos = half_turns(2.0 * relative)
        window[0, pl.ds(start, SUB), :] = 0.54 + 0.46 * (wsign * wcos)
        window[1, pl.ds(start, SUB), :] = squared


def migrate_rows(base, extended, rates_ref, rate_base, weights, window, focus):
    @pl.loop(0, FACTOR // SUB)
    def _(q):
        here = pl.ds(pl.multiple_of(q * SUB, SUB), SUB)
        sums = []
        for c in range(2):
            for r in range(GROUP):
                total = weights[0, here, :] * extended[c, base + r, here, :]
                for s in range(1, LOWER + UPPER + 1):
                    total = total + weights[s, here, :] * extended[c, base + r + s, here, :]
                sums.append(total)
        shape = window[0, here, :]
        squared = window[1, here, :]
        for r in range(GROUP):
            sign, sine, cosine = half_turns(rates_ref[rate_base + r] * squared)
            gain = sign * shape
            real, imag = sums[r] * gain, sums[GROUP + r] * gain
            focus[r, here, :FACTOR] = real * cosine + imag * sine
            focus[r, here, FACTOR:] = imag * cosine - real * sine


def inverse_group(focus, left_ref, right_ref, twist_ref, slow, out_ref):
    for r in range(0, GROUP, 2):
        operand = jnp.concatenate([focus[r], focus[r + 1]], axis=0)
        product = right_product(right_ref, operand)
        rows = []
        for k in range(2):
            part = product[k * FACTOR : (k + 1) * FACTOR]
            rows.append(turned(part[:, :FACTOR], part[:, FACTOR:], twist_ref))
        result = left_product(left_ref, rows[0], rows[1])
        for k in range(2):
            lanes = slice(k * FACTOR, (k + 1) * FACTOR)
            for c in range(2):
                slow[c, pl.ds(r + k, FACTOR, stride=GROUP), :] = result[c * FACTOR : (c + 1) * FACTOR, lanes]
    for c in range(2):
        for n in range(FACTOR):
            out_ref[c, :, n * FACTOR : (n + 1) * FACTOR] = slow[c, n * GROUP : (n + 1) * GROUP, :]


def backward_kernel(
    centroid_ref, shifts_ref, rates_ref, wide_ref, left_ref, right_ref, twist_ref,
    out_ref, extended, weights, window, focus, slow, sems,
):
    step = pl.program_id(0)
    steps = extended.shape[1] // GROUP - (LOWER + UPPER) // GROUP
    lead = GROUP + LOWER + UPPER

    def piece(g):
        rows = pl.ds(0, lead) if g == 0 else pl.ds(lead + (g - 1) * GROUP, GROUP)
        return pltpu.make_async_copy(wide_ref.at[:, rows], extended.at[:, rows], sems.at[g])

    @pl.when(step == 0)
    def _():
        for g in range(steps):
            piece(g).start()
        block = lax.axis_index("row") * rates_ref.shape[0] // BLOCK
        fill_weights(centroid_ref[block], shifts_ref[block], weights, window)

    for g in range(steps):
        @pl.when(step == g)
        def _():
            piece(g).wait()

    base = step * GROUP
    migrate_rows(base, extended, rates_ref, base, weights, window, focus)
    inverse_group(focus, left_ref, right_ref, twist_ref, slow, out_ref)


def backward(centroid, shifts, rates, wide):
    own_rows = wide.shape[1] - LOWER - UPPER
    left, right, twist = tables(True)
    vmem = pl.BlockSpec(memory_space=pltpu.VMEM)
    smem = pl.BlockSpec(memory_space=pltpu.SMEM)
    hbm = pl.BlockSpec(memory_space=pl.ANY)
    return pl.pallas_call(
        backward_kernel,
        grid=(own_rows // GROUP,),
        in_specs=[smem, smem, smem, hbm, vmem, vmem, vmem],
        out_specs=pl.BlockSpec((2, GROUP, PULSES), lambda g: (0, g, 0)),
        out_shape=jax.ShapeDtypeStruct((2, own_rows, PULSES), jnp.float32),
        scratch_shapes=[
            pltpu.VMEM((2, own_rows + LOWER + UPPER, FACTOR, FACTOR), jnp.float32),
            pltpu.VMEM((LOWER + UPPER + 1, FACTOR, FACTOR), jnp.float32),
            pltpu.VMEM((2, FACTOR, FACTOR), jnp.float32),
            pltpu.VMEM((GROUP, FACTOR, 2 * FACTOR), jnp.float32),
            pltpu.VMEM((2, FACTOR * GROUP, FACTOR), jnp.float32),
            pltpu.SemaphoreType.DMA((own_rows // GROUP,)),
        ],
        compiler_params=pltpu.CompilerParams(vmem_limit_bytes=60 * 2**20),
    )(centroid, shifts, rates, wide, left, right, twist)


def gather_kernel(
    devices, raw_ref, left_hbm, right_hbm, twist_hbm, wide_ref,
    left_ref, right_ref, twist_ref, table_sems, landed, extended, slow, send_sem, recv_sems, self_sem, out_sems, rim_send, rim_recv,
):
    me = lax.axis_index("row")
    own_rows = landed.shape[2]
    groups = own_rows // GROUP
    pieces = landed.shape[3] // FACTOR

    fetches = [
        pltpu.make_async_copy(source, target, table_sems.at[i])
        for i, (source, target) in enumerate(
            [(left_hbm, left_ref), (right_hbm, right_ref), (twist_hbm, twist_ref)]
        )
    ]
    for fetch in fetches:
        fetch.start()
    barrier = pltpu.get_barrier_semaphore()

    @pl.loop(1, devices)
    def _(k):
        pl.semaphore_signal(barrier, inc=1, device_id={"row": (me + k) % devices})

    pl.semaphore_wait(barrier, devices - 1)

    own = pltpu.make_async_copy(raw_ref.at[:, pl.ds(me * own_rows, own_rows)], landed.at[:, me], self_sem)
    own.start()
    first = -(-UPPER // GROUP)
    order = list(range(first)) + list(range(groups - 1, first - 1, -1))

    def issue(g):
        @pl.loop(1, devices)
        def _(k):
            peer = (me + k) % devices
            pltpu.make_async_remote_copy(
                src_ref=raw_ref.at[:, pl.ds(peer * own_rows + g * GROUP, GROUP)],
                dst_ref=landed.at[:, me, pl.ds(g * GROUP, GROUP)],
                send_sem=send_sem,
                recv_sem=recv_sems.at[g],
                device_id={"row": peer},
            ).start()

    for g in order[: first + 1]:
        issue(g)

    @pl.when(me == 0)
    def _():
        extended[:, 0:LOWER] = jnp.zeros((2, LOWER, FACTOR, FACTOR), jnp.float32)

    @pl.when(me == devices - 1)
    def _():
        extended[:, LOWER + own_rows :] = jnp.zeros((2, UPPER, FACTOR, FACTOR), jnp.float32)

    own.wait()
    for fetch in fetches:
        fetch.wait()

    def rim_copy(first, count, target, where, slot):
        return pltpu.make_async_remote_copy(
            src_ref=extended.at[:, LOWER + first : LOWER + first + count],
            dst_ref=extended.at[:, where : where + count],
            send_sem=rim_send.at[slot],
            recv_sem=rim_recv.at[slot],
            device_id={"row": target},
        )

    above = rim_copy(0, UPPER, jnp.maximum(me - 1, 0), LOWER + own_rows, 0)
    below = rim_copy(own_rows - LOWER, LOWER, jnp.minimum(me + 1, devices - 1), 0, 1)

    def written(g):
        rows = pl.ds(LOWER + g * GROUP, GROUP)
        return pltpu.make_async_copy(extended.at[:, rows], wide_ref.at[:, rows], out_sems.at[g])

    def arrive_and_transform(g):
        chunk = landed.at[:, 0 : devices - 1, pl.ds(g * GROUP, GROUP)]
        pltpu.make_async_copy(chunk, chunk, recv_sems.at[g]).wait()
        rows = pl.ds(pl.multiple_of(g * GROUP, GROUP), GROUP)
        for c in range(2):
            for d in range(devices):
                for j in range(pieces):
                    start = (d * pieces + j) * GROUP
                    slow[c, start : start + GROUP, :] = landed[c, d, rows, j * FACTOR : (j + 1) * FACTOR]
        for r in range(0, GROUP, 2):
            pair = [
                [slow[c, pl.ds(r + k, FACTOR, stride=GROUP), :] for c in range(2)] for k in range(2)
            ]
            result = forward_pair(pair, left_ref, right_ref, twist_ref)
            for k in range(2):
                part = result[k * FACTOR : (k + 1) * FACTOR]
                extended[0, LOWER + g * GROUP + r + k] = part[:, :FACTOR]
                extended[1, LOWER + g * GROUP + r + k] = part[:, FACTOR:]
        written(g).start()

    @pl.loop(0, first)
    def _(g):
        arrive_and_transform(g)

    @pl.when(me > 0)
    def _():
        above.start()

    for g in order[first + 1 :]:
        issue(g)

    @pl.loop(0, groups - first)
    def _(k):
        arrive_and_transform(groups - 1 - k)

        @pl.when((k == 0) & (me < devices - 1))
        def _():
            below.start()

    everything = landed.at[:, 0 : devices - 1]
    pltpu.make_async_copy(everything, everything, send_sem).wait()

    @pl.when(me > 0)
    def _():
        above.wait_send()
        below.wait_recv()

    @pl.when(me < devices - 1)
    def _():
        below.wait_send()
        above.wait_recv()

    rims = [
        pltpu.make_async_copy(extended.at[:, 0:LOWER], wide_ref.at[:, 0:LOWER], out_sems.at[groups]),
        pltpu.make_async_copy(
            extended.at[:, LOWER + own_rows :], wide_ref.at[:, LOWER + own_rows :], out_sems.at[groups + 1]
        ),
    ]
    for rim in rims:
        rim.start()
    for g in range(groups):
        written(g).wait()
    for rim in rims:
        rim.wait()


def gather_forward(raw, devices):
    own_rows = raw.shape[1] // devices
    share = raw.shape[2]
    groups = own_rows // GROUP
    wide_shape = (2, own_rows + LOWER + UPPER, FACTOR, FACTOR)
    left, right, twist = tables(False)
    hbm = pl.BlockSpec(memory_space=pl.ANY)
    return pl.pallas_call(
        functools.partial(gather_kernel, devices),
        in_specs=[hbm, hbm, hbm, hbm],
        out_specs=hbm,
        out_shape=jax.ShapeDtypeStruct(wide_shape, jnp.float32),
        scratch_shapes=[
            pltpu.VMEM(left.shape, left.dtype),
            pltpu.VMEM(right.shape, right.dtype),
            pltpu.VMEM(twist.shape, twist.dtype),
            pltpu.SemaphoreType.DMA((3,)),
            pltpu.VMEM((2, devices, own_rows, share), jnp.float32),
            pltpu.VMEM(wide_shape, jnp.float32),
            pltpu.VMEM((2, FACTOR * GROUP, FACTOR), jnp.float32),
            pltpu.SemaphoreType.DMA,
            pltpu.SemaphoreType.DMA((groups,)),
            pltpu.SemaphoreType.DMA,
            pltpu.SemaphoreType.DMA((groups + 2,)),
            pltpu.SemaphoreType.DMA((2,)),
            pltpu.SemaphoreType.DMA((2,)),
        ],
        compiler_params=pltpu.CompilerParams(
            collective_id=0, has_side_effects=True, vmem_limit_bytes=58 * 2**20
        ),
    )(raw, left, right, twist)


def per_device(raw_echo, centroid, shifts, chirp_rate):
    devices = lax.axis_size("row")
    own_rows = raw_echo.shape[1] // devices
    assert BLOCK % own_rows == 0 and own_rows % GROUP == 0 and own_rows >= UPPER
    wide = gather_forward(raw_echo, devices)
    return backward(centroid, shifts, chirp_rate, wide)


def solution(mesh):
    return jax.shard_map(
        per_device,
        mesh=mesh,
        in_specs=(P(None, "slab", "row"), P("slab"), P("slab"), P(("slab", "row"))),
        out_specs=P(None, ("slab", "row"), None),
        check_vma=False,
    )
```

```python
import functools
import math

import jax
import jax.numpy as jnp
import numpy as np
from jax import lax
from jax.experimental import pallas as pl
from jax.experimental.pallas import tpu as pltpu
from jax.sharding import PartitionSpec as P

FACTOR = 128
PULSES = FACTOR * FACTOR
BLOCK = 128
MAXSHIFT = 12
TAPS = 4
LOWER = TAPS - 1
UPPER = MAXSHIFT + TAPS - 1
GROUP = 8
SUB = 8


def split(value):
    high = value.astype(jnp.bfloat16)
    low = (value - high.astype(jnp.float32)).astype(jnp.bfloat16)
    return high, low


def tables(inverse):
    grid = np.outer(np.arange(FACTOR), np.arange(FACTOR)).astype(np.float64)
    angle = 2.0 * math.pi * (grid % FACTOR) / FACTOR
    scale = 1.0 / FACTOR if inverse else 1.0
    cosine = np.cos(angle) * scale
    sine = np.sin(angle) * scale * (-1.0 if inverse else 1.0)
    left = np.block([[cosine, sine], [-sine, cosine]]).astype(np.float32)
    right = np.block([[cosine, -sine], [sine, cosine]]).astype(np.float32)
    turn = 2.0 * math.pi * grid / PULSES
    twist = np.stack([np.cos(turn), np.sin(turn) * (1.0 if inverse else -1.0)]).astype(np.float32)

    def pieces(table):
        high = table.astype(jnp.bfloat16)
        low = (table - high.astype(np.float32)).astype(jnp.bfloat16)
        return high, low

    left_high, left_low = pieces(left)
    right_high, right_low = pieces(right)
    left_all = np.concatenate([left_high, left_high, left_low], axis=1)
    right_all = np.concatenate([right_high, right_high, right_low], axis=0)
    return jnp.asarray(left_all), jnp.asarray(right_all), jnp.asarray(twist)


def left_product(left_ref, first, second):
    operand = jnp.concatenate(
        [jnp.concatenate([first[0], second[0]], axis=1), jnp.concatenate([first[1], second[1]], axis=1)],
        axis=0,
    )
    high, low = split(operand)
    stacked = jnp.concatenate([high, low, high], axis=0)
    return jnp.dot(left_ref[...], stacked, preferred_element_type=jnp.float32)


def right_product(right_ref, operand):
    high, low = split(operand)
    stacked = jnp.concatenate([high, low, high], axis=1)
    return jnp.dot(stacked, right_ref[...], preferred_element_type=jnp.float32)


def turned(real, imag, twist_ref):
    return real * twist_ref[0] - imag * twist_ref[1], real * twist_ref[1] + imag * twist_ref[0]


def forward_pair(rows, left_ref, right_ref, twist_ref):
    product = left_product(left_ref, rows[0], rows[1])
    parts = []
    for k in range(2):
        lanes = slice(k * FACTOR, (k + 1) * FACTOR)
        real, imag = turned(product[:FACTOR, lanes], product[FACTOR:, lanes], twist_ref)
        parts.append(jnp.concatenate([real, imag], axis=1))
    return right_product(right_ref, jnp.concatenate(parts, axis=0))


def half_turns(t):
    n = jnp.round(t)
    w = (t - n) * math.pi
    odd = n - 2.0 * jnp.floor(n * 0.5)
    sign = 1.0 - 2.0 * odd
    w2 = w * w
    sine = w * (1.0 + w2 * (-1 / 6 + w2 * (1 / 120 + w2 * (-1 / 5040 + w2 * (1 / 362880 - w2 * (1 / 39916800))))))
    cosine = 1.0 + w2 * (-0.5 + w2 * (1 / 24 + w2 * (-1 / 720 + w2 * (1 / 40320 - w2 * (1 / 3628800)))))
    return sign, sine, cosine


def relative_of(start, center):
    slow = lax.broadcasted_iota(jnp.int32, (SUB, FACTOR), 0) + start
    fast = lax.broadcasted_iota(jnp.int32, (SUB, FACTOR), 1)
    bins = fast * FACTOR + slow
    wrapped = ((bins - center + PULSES // 2) & (PULSES - 1)) - PULSES // 2
    return wrapped.astype(jnp.float32) * (1.0 / PULSES)


def fill_weights(center, shift, weights, window):
    @pl.loop(0, FACTOR // SUB)
    def _(q):
        start = pl.multiple_of(q * SUB, SUB)
        relative = relative_of(start, center)
        squared = relative * relative
        migration = shift.astype(jnp.float32) * 4.0 * squared
        sign, sine, _c = half_turns(migration)
        sine = sign * sine
        sign4, sine4, cosine4 = half_turns(migration * 0.25)
        sine4 = sign4 * sine4
        cosine4 = sign4 * cosine4
        for s in range(-LOWER, UPPER + 1):
            x = s - migration
            zero = x == 0.0
            numerator = sine * ((1.0 if s % 2 else -1.0) / math.pi)
            sinc = jnp.where(zero, 1.0, numerator / jnp.where(zero, 1.0, x))
            taper = 0.5 + (0.5 * math.cos(math.pi * s / 4)) * cosine4 + (0.5 * math.sin(math.pi * s / 4)) * sine4
            value = jnp.where(jnp.abs(x) < TAPS, sinc * taper, 0.0)
            weights[s + LOWER, pl.ds(start, SUB), :] = value
        wsign, _s, wcos = half_turns(2.0 * relative)
        window[0, pl.ds(start, SUB), :] = 0.54 + 0.46 * (wsign * wcos)
        window[1, pl.ds(start, SUB), :] = squared


def migrate_rows(base, extended, rates_ref, rate_base, weights, window, focus):
    @pl.loop(0, FACTOR // SUB)
    def _(q):
        here = pl.ds(pl.multiple_of(q * SUB, SUB), SUB)
        sums = []
        for c in range(2):
            for r in range(GROUP):
                total = weights[0, here, :] * extended[c, base + r, here, :]
                for s in range(1, LOWER + UPPER + 1):
                    total = total + weights[s, here, :] * extended[c, base + r + s, here, :]
                sums.append(total)
        shape = window[0, here, :]
        squared = window[1, here, :]
        for r in range(GROUP):
            sign, sine, cosine = half_turns(rates_ref[rate_base + r] * squared)
            gain = sign * shape
            real, imag = sums[r] * gain, sums[GROUP + r] * gain
            focus[r, here, :FACTOR] = real * cosine + imag * sine
            focus[r, here, FACTOR:] = imag * cosine - real * sine


def inverse_group(focus, left_ref, right_ref, twist_ref, slow, out_ref):
    for r in range(0, GROUP, 2):
        operand = jnp.concatenate([focus[r], focus[r + 1]], axis=0)
        product = right_product(right_ref, operand)
        rows = []
        for k in range(2):
            part = product[k * FACTOR : (k + 1) * FACTOR]
            rows.append(turned(part[:, :FACTOR], part[:, FACTOR:], twist_ref))
        result = left_product(left_ref, rows[0], rows[1])
        for k in range(2):
            lanes = slice(k * FACTOR, (k + 1) * FACTOR)
            for c in range(2):
                slow[c, pl.ds(r + k, FACTOR, stride=GROUP), :] = result[c * FACTOR : (c + 1) * FACTOR, lanes]
    for c in range(2):
        for n in range(FACTOR):
            out_ref[c, :, n * FACTOR : (n + 1) * FACTOR] = slow[c, n * GROUP : (n + 1) * GROUP, :]


def backward_kernel(
    centroid_ref, shifts_ref, rates_ref, wide_ref, left_ref, right_ref, twist_ref,
    out_ref, extended, weights, window, focus, slow, sems,
):
    step = pl.program_id(0)
    steps = extended.shape[1] // GROUP - (LOWER + UPPER) // GROUP
    lead = GROUP + LOWER + UPPER

    def piece(g):
        rows = pl.ds(0, lead) if g == 0 else pl.ds(lead + (g - 1) * GROUP, GROUP)
        return pltpu.make_async_copy(wide_ref.at[:, rows], extended.at[:, rows], sems.at[g])

    @pl.when(step == 0)
    def _():
        for g in range(steps):
            piece(g).start()
        block = lax.axis_index("row") * rates_ref.shape[0] // BLOCK
        fill_weights(centroid_ref[block], shifts_ref[block], weights, window)

    for g in range(steps):
        @pl.when(step == g)
        def _():
            piece(g).wait()

    base = step * GROUP
    migrate_rows(base, extended, rates_ref, base, weights, window, focus)
    inverse_group(focus, left_ref, right_ref, twist_ref, slow, out_ref)


def backward(centroid, shifts, rates, wide):
    own_rows = wide.shape[1] - LOWER - UPPER
    left, right, twist = tables(True)
    vmem = pl.BlockSpec(memory_space=pltpu.VMEM)
    smem = pl.BlockSpec(memory_space=pltpu.SMEM)
    hbm = pl.BlockSpec(memory_space=pl.ANY)
    return pl.pallas_call(
        backward_kernel,
        grid=(own_rows // GROUP,),
        in_specs=[smem, smem, smem, hbm, vmem, vmem, vmem],
        out_specs=pl.BlockSpec((2, GROUP, PULSES), lambda g: (0, g, 0)),
        out_shape=jax.ShapeDtypeStruct((2, own_rows, PULSES), jnp.float32),
        scratch_shapes=[
            pltpu.VMEM((2, own_rows + LOWER + UPPER, FACTOR, FACTOR), jnp.float32),
            pltpu.VMEM((LOWER + UPPER + 1, FACTOR, FACTOR), jnp.float32),
            pltpu.VMEM((2, FACTOR, FACTOR), jnp.float32),
            pltpu.VMEM((GROUP, FACTOR, 2 * FACTOR), jnp.float32),
            pltpu.VMEM((2, FACTOR * GROUP, FACTOR), jnp.float32),
            pltpu.SemaphoreType.DMA((own_rows // GROUP,)),
        ],
        compiler_params=pltpu.CompilerParams(vmem_limit_bytes=60 * 2**20),
    )(centroid, shifts, rates, wide, left, right, twist)


def gather_kernel(
    devices, raw_ref, left_hbm, right_hbm, twist_hbm, wide_ref,
    left_ref, right_ref, twist_ref, table_sems, landed, extended, slow, send_sem, recv_sems, self_sem, out_sems, rim_send, rim_recv,
):
    me = lax.axis_index("row")
    own_rows = landed.shape[2]
    groups = own_rows // GROUP
    pieces = landed.shape[3] // FACTOR

    fetches = [
        pltpu.make_async_copy(source, target, table_sems.at[i])
        for i, (source, target) in enumerate(
            [(left_hbm, left_ref), (right_hbm, right_ref), (twist_hbm, twist_ref)]
        )
    ]
    for fetch in fetches:
        fetch.start()
    barrier = pltpu.get_barrier_semaphore()

    @pl.loop(1, devices)
    def _(k):
        pl.semaphore_signal(barrier, inc=1, device_id={"row": (me + k) % devices})

    pl.semaphore_wait(barrier, devices - 1)

    own = pltpu.make_async_copy(raw_ref.at[:, pl.ds(me * own_rows, own_rows)], landed.at[:, me], self_sem)
    own.start()
    first = -(-UPPER // GROUP)
    order = list(range(first)) + list(range(groups - 1, first - 1, -1))

    def issue(g):
        @pl.loop(1, devices)
        def _(k):
            peer = (me + k) % devices
            pltpu.make_async_remote_copy(
                src_ref=raw_ref.at[:, pl.ds(peer * own_rows + g * GROUP, GROUP)],
                dst_ref=landed.at[:, me, pl.ds(g * GROUP, GROUP)],
                send_sem=send_sem,
                recv_sem=recv_sems.at[g],
                device_id={"row": peer},
            ).start()

    for g in order[:first]:
        issue(g)

    @pl.when(me == 0)
    def _():
        extended[:, 0:LOWER] = jnp.zeros((2, LOWER, FACTOR, FACTOR), jnp.float32)

    @pl.when(me == devices - 1)
    def _():
        extended[:, LOWER + own_rows :] = jnp.zeros((2, UPPER, FACTOR, FACTOR), jnp.float32)

    own.wait()
    for fetch in fetches:
        fetch.wait()

    def rim_copy(first, count, target, where, slot):
        return pltpu.make_async_remote_copy(
            src_ref=extended.at[:, LOWER + first : LOWER + first + count],
            dst_ref=extended.at[:, where : where + count],
            send_sem=rim_send.at[slot],
            recv_sem=rim_recv.at[slot],
            device_id={"row": target},
        )

    above = rim_copy(0, UPPER, jnp.maximum(me - 1, 0), LOWER + own_rows, 0)
    below = rim_copy(own_rows - LOWER, LOWER, jnp.minimum(me + 1, devices - 1), 0, 1)

    def written(g):
        rows = pl.ds(LOWER + g * GROUP, GROUP)
        return pltpu.make_async_copy(extended.at[:, rows], wide_ref.at[:, rows], out_sems.at[g])

    def arrive_and_transform(g):
        chunk = landed.at[:, 0 : devices - 1, pl.ds(g * GROUP, GROUP)]
        pltpu.make_async_copy(chunk, chunk, recv_sems.at[g]).wait()
        rows = pl.ds(pl.multiple_of(g * GROUP, GROUP), GROUP)
        for c in range(2):
            for d in range(devices):
                for j in range(pieces):
                    start = (d * pieces + j) * GROUP
                    slow[c, start : start + GROUP, :] = landed[c, d, rows, j * FACTOR : (j + 1) * FACTOR]
        for r in range(0, GROUP, 2):
            pair = [
                [slow[c, pl.ds(r + k, FACTOR, stride=GROUP), :] for c in range(2)] for k in range(2)
            ]
            result = forward_pair(pair, left_ref, right_ref, twist_ref)
            for k in range(2):
                part = result[k * FACTOR : (k + 1) * FACTOR]
                extended[0, LOWER + g * GROUP + r + k] = part[:, :FACTOR]
                extended[1, LOWER + g * GROUP + r + k] = part[:, FACTOR:]
        written(g).start()

    @pl.loop(0, first)
    def _(g):
        arrive_and_transform(g)

    @pl.when(me > 0)
    def _():
        above.start()

    for g in order[first:]:
        issue(g)

    @pl.loop(0, groups - first)
    def _(k):
        arrive_and_transform(groups - 1 - k)

        @pl.when((k == 0) & (me < devices - 1))
        def _():
            below.start()

    everything = landed.at[:, 0 : devices - 1]
    pltpu.make_async_copy(everything, everything, send_sem).wait()

    @pl.when(me > 0)
    def _():
        above.wait_send()
        below.wait_recv()

    @pl.when(me < devices - 1)
    def _():
        below.wait_send()
        above.wait_recv()

    rims = [
        pltpu.make_async_copy(extended.at[:, 0:LOWER], wide_ref.at[:, 0:LOWER], out_sems.at[groups]),
        pltpu.make_async_copy(
            extended.at[:, LOWER + own_rows :], wide_ref.at[:, LOWER + own_rows :], out_sems.at[groups + 1]
        ),
    ]
    for rim in rims:
        rim.start()
    for g in range(groups):
        written(g).wait()
    for rim in rims:
        rim.wait()


def gather_forward(raw, devices):
    own_rows = raw.shape[1] // devices
    share = raw.shape[2]
    groups = own_rows // GROUP
    wide_shape = (2, own_rows + LOWER + UPPER, FACTOR, FACTOR)
    left, right, twist = tables(False)
    hbm = pl.BlockSpec(memory_space=pl.ANY)
    return pl.pallas_call(
        functools.partial(gather_kernel, devices),
        in_specs=[hbm, hbm, hbm, hbm],
        out_specs=hbm,
        out_shape=jax.ShapeDtypeStruct(wide_shape, jnp.float32),
        scratch_shapes=[
            pltpu.VMEM(left.shape, left.dtype),
            pltpu.VMEM(right.shape, right.dtype),
            pltpu.VMEM(twist.shape, twist.dtype),
            pltpu.SemaphoreType.DMA((3,)),
            pltpu.VMEM((2, devices, own_rows, share), jnp.float32),
            pltpu.VMEM(wide_shape, jnp.float32),
            pltpu.VMEM((2, FACTOR * GROUP, FACTOR), jnp.float32),
            pltpu.SemaphoreType.DMA,
            pltpu.SemaphoreType.DMA((groups,)),
            pltpu.SemaphoreType.DMA,
            pltpu.SemaphoreType.DMA((groups + 2,)),
            pltpu.SemaphoreType.DMA((2,)),
            pltpu.SemaphoreType.DMA((2,)),
        ],
        compiler_params=pltpu.CompilerParams(
            collective_id=0, has_side_effects=True, vmem_limit_bytes=58 * 2**20
        ),
    )(raw, left, right, twist)


def per_device(raw_echo, centroid, shifts, chirp_rate):
    devices = lax.axis_size("row")
    own_rows = raw_echo.shape[1] // devices
    assert BLOCK % own_rows == 0 and own_rows % GROUP == 0 and own_rows >= UPPER
    wide = gather_forward(raw_echo, devices)
    return backward(centroid, shifts, chirp_rate, wide)


def solution(mesh):
    return jax.shard_map(
        per_device,
        mesh=mesh,
        in_specs=(P(None, "slab", "row"), P("slab"), P("slab"), P(("slab", "row"))),
        out_specs=P(None, ("slab", "row"), None),
        check_vma=False,
    )
```
